8 devices in a mesh: dp: 1 (over z), tp: 8 (over x, y, core).
Axes of the slice: x: 2, y: 2, z: 1, core: 2. Of those that a mesh axis runs over, the one named last changes fastest.
Arguments:
- x: bfloat16 [4, 512, 7168], P('dp')
- gain_a: bfloat16 [7168], replicated
- wq: bfloat16 [7168, 7168], P(None, 'tp')
- wk: bfloat16 [7168, 1024], P(None, 'tp')
- wv: bfloat16 [7168, 1024], P(None, 'tp')
- wo: bfloat16 [7168, 7168], P('tp')
- gain_m: bfloat16 [7168], replicated
- w_gate: bfloat16 [7168, 20480], P(None, 'tp')
- w_up: bfloat16 [7168, 20480], P(None, 'tp')
- w_down: bfloat16 [20480, 7168], P('tp')
Outputs:
- output: bfloat16 [4, 512, 7168], P('dp')
All inputs are finite; a program needn't handle non-finite values.
Results may differ from the reference program's by a relative error of at most 0.017.
Values are sent between devices in bfloat16 or wider.
A program may use at most 2 GiB of HBM per device.

```python
import jax
import jax.numpy as jnp
from jax import lax

SEQUENCES = 4
TOKENS = 512
D = 7168
HEADS = 56
KV_HEADS = 8
HEAD = 128
FF = 20480
THETA = 10000


def setup_inputs(seed: int = 0, part: int = 0) -> dict:
    kx, ka, km, kq, kk, kv, ko, kg, ku, kd = jax.random.split(jax.random.key(seed), 10)

    def weights(key, rows, columns):
        return jax.random.normal(key, (rows, columns), jnp.float32) * rows**-0.5

    drawn = {
        "x": jax.random.normal(jax.random.fold_in(kx, part), (SEQUENCES, TOKENS, D), jnp.float32),
        "gain_a": 1 + 0.1 * jax.random.normal(ka, (D,), jnp.float32),
        "wq": 2 * weights(kq, D, HEADS * HEAD),
        "wk": 2 * weights(kk, D, KV_HEADS * HEAD),
        "wv": 4 * weights(kv, D, KV_HEADS * HEAD),
        "wo": weights(ko, HEADS * HEAD, D),
        "gain_m": 1 + 0.1 * jax.random.normal(km, (D,), jnp.float32),
        "w_gate": weights(kg, D, FF),
        "w_up": weights(ku, D, FF),
        "w_down": 3 * weights(kd, FF, D),
    }
    return {k: v.astype(jnp.bfloat16) for k, v in drawn.items()}


def normed(x, gain):
    wide = x.astype(jnp.float32)
    scale = lax.rsqrt(jnp.mean(wide * wide, -1, keepdims=True) + 1e-6)
    return (wide * scale * gain.astype(jnp.float32)).astype(jnp.bfloat16)


def turned(t, place, theta):
    half = t.shape[-1] // 2
    angle = place.astype(jnp.float32)[:, None] * theta ** (-jnp.arange(half, dtype=jnp.float32) / half)
    cos, sin = jnp.cos(angle)[:, None], jnp.sin(angle)[:, None]
    a, b = t[..., :half].astype(jnp.float32), t[..., half:].astype(jnp.float32)
    return jnp.concatenate([a * cos - b * sin, b * cos + a * sin], -1).astype(jnp.bfloat16)


def matmul(a, w):
    return jnp.dot(a, w, preferred_element_type=jnp.float32).astype(jnp.bfloat16)


def einsum(form, a, b):
    return jnp.einsum(form, a.astype(jnp.float32), b.astype(jnp.float32))


def attention(q, k, v):
    scores = einsum("tgsd,ugd->gstu", q, k) * q.shape[-1] ** -0.5
    token = jnp.arange(q.shape[0])
    scores = jnp.where(token[:, None] >= token, scores, -jnp.inf)
    weights = jax.nn.softmax(scores, -1).astype(jnp.bfloat16)
    return einsum("gstu,ugd->tgsd", weights, v).astype(jnp.bfloat16)


def one(x, gain_a, wq, wk, wv, wo, gain_m, w_gate, w_up, w_down):
    rows = x.shape[0]
    a, place = normed(x, gain_a), jnp.arange(rows)
    k = turned(matmul(a, wk).reshape(rows, -1, HEAD), place, THETA)
    q = turned(matmul(a, wq).reshape(rows, -1, HEAD), place, THETA).reshape(rows, k.shape[1], -1, HEAD)
    v = matmul(a, wv).reshape(rows, -1, HEAD)
    seen = attention(q, k, v).reshape(rows, -1)
    h = (x.astype(jnp.float32) + jnp.dot(seen, wo, preferred_element_type=jnp.float32)).astype(jnp.bfloat16)
    b = normed(h, gain_m)
    gate = jnp.dot(b, w_gate, preferred_element_type=jnp.float32)
    up = jnp.dot(b, w_up, preferred_element_type=jnp.float32)
    hidden = (jax.nn.silu(gate) * up).astype(jnp.bfloat16)
    return (h.astype(jnp.float32) + jnp.dot(hidden, w_down, preferred_element_type=jnp.float32)).astype(jnp.bfloat16)


def reference(x, gain_a, wq, wk, wv, wo, gain_m, w_gate, w_up, w_down):
    return lax.map(lambda sequence: one(sequence, gain_a, wq, wk, wv, wo, gain_m, w_gate, w_up, w_down), x)
```

```python
import functools

import jax
import jax.numpy as jnp
from jax import lax
from jax.experimental import pallas as pl
from jax.experimental.pallas import tpu as pltpu
from jax.sharding import PartitionSpec as P

HEAD = 128
THETA = 10000
LOG2E = 1.4426950408889634
HIDDEN = -1e30
VMEM = 60 * 2**20
MESH = pl.DeviceIdType.MESH
F32, BF16 = jnp.float32, jnp.bfloat16


def _dot(a, b, ca=1, cb=0):
    return lax.dot_general(a, b, (((ca,), (cb,)), ((), ())), preferred_element_type=F32)


def _turn(t, cos, sin):
    t = t.astype(BF16).astype(F32)
    return (t * cos + pltpu.roll(t, HEAD // 2, 1) * sin).astype(BF16)


def _attend_kernel(x_ref, gain_ref, wk_ref, wv_ref, wq_ref, cos_ref, sin_ref, o_ref, a_s, k_s, vt_s):
    rows, bq = x_ref.shape[1], 256
    step = pl.program_id(0)

    @pl.when(step == 0)
    def _():
        gain = gain_ref[...].astype(F32)

        @pl.loop(0, rows // 64)
        def _(i):
            here = pl.ds(pl.multiple_of(i * 64, 64), 64)
            wide = x_ref[0, here, :].astype(F32)
            scale = lax.rsqrt(jnp.mean(wide * wide, -1, keepdims=True) + 1e-6)
            a_s[here, :] = (wide * scale * gain).astype(BF16)

        kv = _dot(a_s[...], jnp.concatenate([wk_ref[...], wv_ref[...]], axis=1))
        k_s[...] = _turn(kv[:, :HEAD], cos_ref[...], sin_ref[...])
        vt_s[...] = kv[:, HEAD:].T.astype(BF16)

    @pl.when(step > 0)
    def _():
        e = HEAD**-0.5 * LOG2E
        q2 = _dot(a_s[...], wq_ref[...])
        seen = lax.broadcasted_iota(jnp.int32, (bq, bq), 0) <= lax.broadcasted_iota(jnp.int32, (bq, bq), 1)
        for n in range(2):
            q = _turn(q2[:, n * HEAD : (n + 1) * HEAD], cos_ref[...], sin_ref[...])
            for at in range(0, rows, bq):
                mine = q[at : at + bq]
                s = [_dot(k_s[j : j + bq, :], mine, 1, 1) for j in range(0, at + bq, bq)]
                s[-1] = jnp.where(seen, s[-1], HIDDEN)
                top = functools.reduce(jnp.maximum, [t.max(axis=0, keepdims=True) for t in s])
                p = [jnp.exp2((t - top) * e) for t in s]
                total = sum(t.sum(axis=0, keepdims=True) for t in p)
                out = sum(_dot(vt_s[:, j * bq : (j + 1) * bq], t.astype(BF16)) for j, t in enumerate(p))
                o_ref[at : at + bq, n * HEAD : (n + 1) * HEAD] = (out * (1 / total)).T.astype(BF16)


def attended(x, c, gain, wq, wk, wv, cos, sin):
    rows, d = x.shape[1:]
    width = wq.shape[1]
    steps = pl.cdiv(width, 2 * HEAD)
    later = lambda s: (0, jnp.maximum(s - 1, 0))
    fixed = lambda s: (0, 0)
    return pl.pallas_call(
        _attend_kernel,
        grid=(steps + 1,),
        in_specs=[
            pl.BlockSpec((1, rows, d), lambda s: (c, 0, 0)),
            pl.BlockSpec((1, d), fixed),
            pl.BlockSpec((d, HEAD), fixed),
            pl.BlockSpec((d, HEAD), fixed),
            pl.BlockSpec((d, 2 * HEAD), later),
            pl.BlockSpec((rows, HEAD), fixed),
            pl.BlockSpec((rows, HEAD), fixed),
        ],
        out_specs=pl.BlockSpec((rows, 2 * HEAD), later),
        out_shape=jax.ShapeDtypeStruct((rows, width), BF16),
        scratch_shapes=[pltpu.VMEM((rows, d), BF16), pltpu.VMEM((rows, HEAD), BF16), pltpu.VMEM((HEAD, rows), BF16)],
        compiler_params=pltpu.CompilerParams(dimension_semantics=("arbitrary",), vmem_limit_bytes=VMEM),
        cost_estimate=pl.CostEstimate(flops=2 * rows * d * (width + 2 * HEAD) + 4 * rows * rows * width, transcendentals=rows * rows * width // HEAD,
                                      bytes_accessed=2 * (rows * d + d * (width + 2 * HEAD))),
        name="attended",
    )(x, gain, wk, wv, wq, cos, sin)


def _gated_kernel(b_ref, g_ref, u_ref, o_ref):
    gate = _dot(b_ref[...], g_ref[...])
    up = _dot(b_ref[...], u_ref[...])
    o_ref[...] = (jax.nn.silu(gate) * up).astype(BF16)


def gated(b, w_gate, w_up, tile=256):
    rows, d = b.shape
    width = w_gate.shape[1]
    columns = pl.BlockSpec((d, tile), lambda j: (0, j))
    return pl.pallas_call(
        _gated_kernel,
        grid=(width // tile,),
        in_specs=[pl.BlockSpec((rows, d), lambda j: (0, 0)), columns, columns],
        out_specs=pl.BlockSpec((rows, tile), lambda j: (0, j)),
        out_shape=jax.ShapeDtypeStruct((rows, width), BF16),
        compiler_params=pltpu.CompilerParams(dimension_semantics=("arbitrary",), vmem_limit_bytes=VMEM),
        cost_estimate=pl.CostEstimate(flops=4 * rows * d * width, transcendentals=rows * width, bytes_accessed=2 * (rows * d + 2 * d * width)),
        name="gated",
    )(b, w_gate, w_up)


LAGS = (1, 3, 5)


def _reduced_kernel(a_ref, w_ref, res_ref, gain_ref, h_ref, *rest, norm):
    b_ref, rest = (rest[0], rest[1:]) if norm else (None, rest)
    rows_s, kept0, kept1, kept2, out0, in0, out1, in1, out2, in2, sent0, came0, sent1, came1, sent2, came2 = rest
    unit = a_ref.shape[0] // 16
    half = 8 * unit
    tile = w_ref.shape[1]
    n = out0.shape[0]
    j = pl.program_id(0)
    me = lax.axis_index("tp")
    x, y, core = me // 4, lax.rem(me // 2, 2), lax.rem(me, 2)
    mate, over_x, over_y = me + 1 - 2 * core, me + 4 - 8 * x, me + 2 - 4 * y

    def remote(src, dst, sent, came, to):
        return pltpu.make_async_remote_copy(src, dst, sent, came, device_id={"tp": to}, device_id_type=MESH)

    def stage0(t):
        return [remote(out0.at[t], in0.at[t], sent0.at[t], came0.at[t], mate)]

    def stage1(t):
        return [remote(out1.at[t, p], in1.at[t, p], sent1.at[t, p], came1.at[t, p], to) for p, to in enumerate((over_x, over_y))]

    def stage2(t):
        return [remote(out2.at[t, p], in2.at[t, p], sent2.at[t, p], came2.at[t, p], to) for p, to in enumerate((over_y, over_x))]

    @pl.when(j == 0)
    def _():
        barrier = pltpu.get_barrier_semaphore()
        for to in (mate, over_x, over_y):
            pl.semaphore_signal(barrier, 1, device_id={"tp": to}, device_id_type=MESH)
        order = [(1 - x, 1 - y, 0), (1 - x, y, 0), (x, 1 - y, 0), (x, y, 0), (1 - x, 1 - y, 1), (x, 1 - y, 1), (1 - x, y, 1), (x, y, 1)]
        for i, (xx, yy, part) in enumerate(order):
            for k, cc in enumerate((1 - core, core)):
                at = pl.multiple_of((((xx * 2 + yy) * 2 + cc) * 2 + part) * unit, unit)
                rows_s[k * half + i * unit : k * half + (i + 1) * unit, :] = a_ref[pl.ds(at, unit), :]
        pl.semaphore_wait(barrier, 3)

    @pl.when(j < n)
    def _():
        both = _dot(rows_s[...], w_ref[...])
        out0[j] = both[:half].astype(BF16)
        for c in stage0(j):
            c.start()
        kept0[lax.rem(j, LAGS[0] + 1)] = both[half:]

    @pl.when((j >= LAGS[0]) & (j < n + LAGS[0]))
    def _():
        t = j - LAGS[0]
        for c in stage0(t):
            c.wait_recv()
        total = kept0[lax.rem(t, LAGS[0] + 1)] + in0[t].astype(F32)
        for p in range(2):
            out1[t, p] = total[4 * p * unit : (4 * p + 2) * unit].astype(BF16)
            kept1[lax.rem(t, 4), p] = total[(4 * p + 2) * unit : (4 * p + 4) * unit]
        for c in stage1(t):
            c.start()

    @pl.when((j >= LAGS[1]) & (j < n + LAGS[1]))
    def _():
        t = j - LAGS[1]
        for c in stage1(t):
            c.wait_recv()
        for p in range(2):
            total = kept1[lax.rem(t, 4), p] + in1[t, p].astype(F32)
            out2[t, p] = total[:unit].astype(BF16)
            kept2[lax.rem(t, 4), p] = total[unit:]
        for c in stage2(t):
            c.start()

    @pl.when(j >= LAGS[2])
    def _():
        t = j - LAGS[2]
        for c in stage2(t):
            c.wait_recv()
        columns = pl.ds(pl.multiple_of(t * tile, tile), tile)
        for p in range(2):
            total = kept2[lax.rem(t, 4), p] + in2[t, p].astype(F32)
            here = slice(p * unit, (p + 1) * unit)
            h_ref[here, columns] = (res_ref[here, columns].astype(F32) + total).astype(BF16)

    @pl.when(j == pl.num_programs(0) - 1)
    def _():
        if norm:
            wide = h_ref[...].astype(F32)
            scale = lax.rsqrt(jnp.mean(wide * wide, -1, keepdims=True) + 1e-6)
            b_ref[...] = (wide * scale * gain_ref[...].astype(F32)).astype(BF16)

        @pl.loop(0, n)
        def _(t):
            for c in stage0(t) + stage1(t) + stage2(t):
                c.wait_send()


def reduced(a, w, res, gain, tile, norm, collective_id):
    rows, k = a.shape
    d = w.shape[1]
    n, unit = d // tile, rows // 16
    fixed = lambda j: (0, 0)
    mine = jax.ShapeDtypeStruct((2 * unit, d), BF16)
    return pl.pallas_call(
        functools.partial(_reduced_kernel, norm=norm),
        grid=(n + LAGS[2],),
        in_specs=[pl.BlockSpec((rows, k), fixed), pl.BlockSpec((k, tile), lambda j: (0, jnp.minimum(j, n - 1))),
                  pl.BlockSpec((2 * unit, d), fixed), pl.BlockSpec((1, d), fixed)],
        out_specs=[pl.BlockSpec((2 * unit, d), fixed)] * (1 + norm),
        out_shape=[mine] * (1 + norm),
        scratch_shapes=[
            pltpu.VMEM((rows, k), BF16),
            pltpu.VMEM((LAGS[0] + 1, 8 * unit, tile), F32),
            pltpu.VMEM((4, 2, 2 * unit, tile), F32),
            pltpu.VMEM((4, 2, unit, tile), F32),
            pltpu.VMEM((n, 8 * unit, tile), BF16),
            pltpu.VMEM((n, 8 * unit, tile), BF16),
            pltpu.VMEM((n, 2, 2 * unit, tile), BF16),
            pltpu.VMEM((n, 2, 2 * unit, tile), BF16),
            pltpu.VMEM((n, 2, unit, tile), BF16),
            pltpu.VMEM((n, 2, unit, tile), BF16),
            pltpu.SemaphoreType.DMA((n,)),
            pltpu.SemaphoreType.DMA((n,)),
            pltpu.SemaphoreType.DMA((n, 2)),
            pltpu.SemaphoreType.DMA((n, 2)),
            pltpu.SemaphoreType.DMA((n, 2)),
            pltpu.SemaphoreType.DMA((n, 2)),
        ],
        compiler_params=pltpu.CompilerParams(dimension_semantics=("arbitrary",), vmem_limit_bytes=VMEM, collective_id=collective_id,
                                             has_side_effects=True),
        cost_estimate=pl.CostEstimate(flops=max(2 * rows * k * d, 2 * rows * 2560 * d), transcendentals=0, bytes_accessed=2 * (rows * k + k * d) + rows * d * 2),
        name=f"reduced{collective_id}",
    )(a, w, res, gain)


def _place_kernel(*refs):
    refs[-1][0] = refs[0][...]


def placed(piece, whole, c, chunks):
    rows, d = piece.shape
    block = 64
    more = [] if whole is None else [whole]
    return pl.pallas_call(
        _place_kernel,
        grid=(rows // block,),
        in_specs=[pl.BlockSpec((block, d), lambda i: (i, 0))] + [pl.BlockSpec(memory_space=pl.ANY)] * len(more),
        out_specs=pl.BlockSpec((1, block, d), lambda i: (c, i, 0)),
        out_shape=jax.ShapeDtypeStruct((chunks, rows, d), piece.dtype),
        input_output_aliases={1: 0} if more else {},
        compiler_params=pltpu.CompilerParams(dimension_semantics=("arbitrary",), vmem_limit_bytes=VMEM),
        cost_estimate=pl.CostEstimate(flops=rows * d * 64, transcendentals=0, bytes_accessed=4 * rows * d),
        name="placed",
    )(piece, *more)


def solution(mesh):
    n = mesh.shape["tp"]

    def step(x, gain_a, wq, wk, wv, wo, gain_m, w_gate, w_up, w_down):
        chunks, rows, d = x.shape
        half = HEAD // 2
        angle = jnp.arange(rows).astype(F32)[:, None] * THETA ** (-jnp.arange(half, dtype=F32) / half)
        cos, sin = jnp.cos(angle), jnp.sin(angle)
        cos, sin = jnp.concatenate([cos, cos], -1), jnp.concatenate([-sin, sin], -1)
        gain_a, gain_m = gain_a.reshape(1, d), gain_m.reshape(1, d)
        mine = lax.dynamic_slice(x, (0, lax.axis_index("tp") * (rows // n), 0), (chunks, rows // n, d))
        own, wholes = [], []
        for c in range(chunks):
            seen = attended(x, c, gain_a, wq, wk, wv, cos, sin)
            h, b = reduced(seen, wo, mine[c], gain_m, 512, True, 0)
            own.append(h)
            wholes.append(lax.all_gather(b, "tp", axis=0, tiled=True))
        y = None
        for c in range(chunks):
            hidden = gated(wholes[c], w_gate, w_up)
            (piece,) = reduced(hidden, w_down, own[c], gain_m, 512, False, 1)
            y = placed(lax.all_gather(piece, "tp", axis=0, tiled=True), y, c, chunks)
        return y

    tokens, whole, columns, rows_of = P("dp", None, None), P(None), P(None, "tp"), P("tp", None)
    return jax.shard_map(
        step,
        mesh=mesh,
        in_specs=(tokens, whole, columns, columns, columns, rows_of, whole, columns, columns, rows_of),
        out_specs=tokens,
        check_vma=False,
    )
```

```python
import functools

import jax
import jax.numpy as jnp
from jax import lax
from jax.experimental import pallas as pl
from jax.experimental.pallas import tpu as pltpu
from jax.sharding import PartitionSpec as P

HEAD = 128
THETA = 10000
LOG2E = 1.4426950408889634
HIDDEN = -1e30
VMEM = 60 * 2**20
MESH = pl.DeviceIdType.MESH
F32, BF16 = jnp.float32, jnp.bfloat16


def _dot(a, b, ca=1, cb=0):
    return lax.dot_general(a, b, (((ca,), (cb,)), ((), ())), preferred_element_type=F32)


def _neighbours():
    me = lax.axis_index("tp")
    x, y, core = me // 4, lax.rem(me // 2, 2), lax.rem(me, 2)
    return x, y, core, me + 1 - 2 * core, me + 4 - 8 * x, me + 2 - 4 * y


def _remote(src, dst, sent, came, to):
    return pltpu.make_async_remote_copy(src, dst, sent, came, device_id={"tp": to}, device_id_type=MESH)


def _normed(h, gain):
    wide = h.astype(F32)
    scale = lax.rsqrt(jnp.mean(wide * wide, -1, keepdims=True) + 1e-6)
    return (wide * scale * gain.astype(F32)).astype(BF16)


def _turn(t, cos, sin):
    t = t.astype(BF16).astype(F32)
    return (t * cos + pltpu.roll(t, HEAD // 2, 1) * sin).astype(BF16)


def _attend_first(take, gain_ref, wkv, cos_ref, sin_ref, a_s, k_s, vt_s):
    @pl.loop(0, a_s.shape[0] // 64)
    def _(i):
        here = pl.ds(pl.multiple_of(i * 64, 64), 64)
        a_s[here, :] = _normed(take(here), gain_ref[...])

    kv = _dot(a_s[...], wkv())
    k_s[...] = _turn(kv[:, :HEAD], cos_ref[...], sin_ref[...])
    vt_s[...] = kv[:, HEAD:].T.astype(BF16)


def _attend_pair(wq, cos_ref, sin_ref, o_ref, a_s, k_s, vt_s):
    rows, bq = a_s.shape[0], 256
    e = HEAD**-0.5 * LOG2E
    q2 = _dot(a_s[...], wq)
    seen = lax.broadcasted_iota(jnp.int32, (bq, bq), 0) <= lax.broadcasted_iota(jnp.int32, (bq, bq), 1)
    for n in range(2):
        q = _turn(q2[:, n * HEAD : (n + 1) * HEAD], cos_ref[...], sin_ref[...])
        for at in range(0, rows, bq):
            mine = q[at : at + bq]
            s = [_dot(k_s[j : j + bq, :], mine, 1, 1) for j in range(0, at + bq, bq)]
            s[-1] = jnp.where(seen, s[-1], HIDDEN)
            top = functools.reduce(jnp.maximum, [t.max(axis=0, keepdims=True) for t in s])
            p = [jnp.exp2((t - top) * e) for t in s]
            total = sum(t.sum(axis=0, keepdims=True) for t in p)
            sums = sum(_dot(vt_s[:, j * bq : (j + 1) * bq], t.astype(BF16)) for j, t in enumerate(p))
            o_ref[at : at + bq, n * HEAD : (n + 1) * HEAD] = (sums * (1 / total)).T.astype(BF16)


def _attend_kernel(x_ref, gain_ref, wk_ref, wv_ref, wq_ref, cos_ref, sin_ref, o_ref, a_s, k_s, vt_s):
    step = pl.program_id(0)

    @pl.when(step == 0)
    def _():
        wkv = lambda: jnp.concatenate([wk_ref[...], wv_ref[...]], axis=1)
        _attend_first(lambda here: x_ref[0, here, :], gain_ref, wkv, cos_ref, sin_ref, a_s, k_s, vt_s)

    @pl.when(step > 0)
    def _():
        _attend_pair(wq_ref[...], cos_ref, sin_ref, o_ref, a_s, k_s, vt_s)


def attended(x, c, gain, wq, wk, wv, cos, sin):
    rows, d = x.shape[1:]
    width = wq.shape[1]
    steps = pl.cdiv(width, 2 * HEAD) + 1
    later = lambda j: (0, jnp.maximum(j - 1, 0))
    fixed = lambda j: (0, 0)
    return pl.pallas_call(
        _attend_kernel,
        grid=(steps,),
        in_specs=[pl.BlockSpec((1, rows, d), lambda j: (c, 0, 0)), pl.BlockSpec((1, d), fixed), pl.BlockSpec((d, HEAD), fixed),
                  pl.BlockSpec((d, HEAD), fixed), pl.BlockSpec((d, 2 * HEAD), later), pl.BlockSpec((rows, HEAD), fixed), pl.BlockSpec((rows, HEAD), fixed)],
        out_specs=pl.BlockSpec((rows, 2 * HEAD), later),
        out_shape=jax.ShapeDtypeStruct((rows, width), BF16),
        scratch_shapes=[pltpu.VMEM((rows, d), BF16), pltpu.VMEM((rows, HEAD), BF16), pltpu.VMEM((HEAD, rows), BF16)],
        compiler_params=pltpu.CompilerParams(dimension_semantics=("arbitrary",), vmem_limit_bytes=VMEM),
        cost_estimate=pl.CostEstimate(flops=2 * rows * d * (width + 2 * HEAD) + 4 * rows * rows * width, transcendentals=0, bytes_accessed=4 * rows * d),
        name="attended",
    )(x, gain, wk, wv, wq, cos, sin)


LAGS = (1, 3, 5)


def _reduced_kernel(a_ref, w_ref, res_ref, gain_ref, h_ref, *rest, norm):
    b_ref, rest = (rest[0], rest[1:]) if norm else (None, rest)
    rows_s, kept0, kept1, kept2, out0, in0, out1, in1, out2, in2, sent0, came0, sent1, came1, sent2, came2 = rest
    unit = a_ref.shape[0] // 16
    half = 8 * unit
    tile = w_ref.shape[1]
    n = out0.shape[0]
    j = pl.program_id(0)
    me = lax.axis_index("tp")
    x, y, core = me // 4, lax.rem(me // 2, 2), lax.rem(me, 2)
    mate, over_x, over_y = me + 1 - 2 * core, me + 4 - 8 * x, me + 2 - 4 * y

    def remote(src, dst, sent, came, to):
        return pltpu.make_async_remote_copy(src, dst, sent, came, device_id={"tp": to}, device_id_type=MESH)

    def stage0(t):
        return [remote(out0.at[t], in0.at[t], sent0.at[t], came0.at[t], mate)]

    def stage1(t):
        return [remote(out1.at[t, p], in1.at[t, p], sent1.at[t, p], came1.at[t, p], to) for p, to in enumerate((over_x, over_y))]

    def stage2(t):
        return [remote(out2.at[t, p], in2.at[t, p], sent2.at[t, p], came2.at[t, p], to) for p, to in enumerate((over_y, over_x))]

    @pl.when(j == 0)
    def _():
        barrier = pltpu.get_barrier_semaphore()
        for to in (mate, over_x, over_y):
            pl.semaphore_signal(barrier, 1, device_id={"tp": to}, device_id_type=MESH)
        order = [(1 - x, 1 - y, 0), (1 - x, y, 0), (x, 1 - y, 0), (x, y, 0), (1 - x, 1 - y, 1), (x, 1 - y, 1), (1 - x, y, 1), (x, y, 1)]
        for i, (xx, yy, part) in enumerate(order):
            for k, cc in enumerate((1 - core, core)):
                at = pl.multiple_of((((xx * 2 + yy) * 2 + cc) * 2 + part) * unit, unit)
                rows_s[k * half + i * unit : k * half + (i + 1) * unit, :] = a_ref[pl.ds(at, unit), :]
        pl.semaphore_wait(barrier, 3)

    @pl.when(j < n)
    def _():
        both = _dot(rows_s[...], w_ref[...])
        out0[j] = both[:half].astype(BF16)
        for c in stage0(j):
            c.start()
        kept0[lax.rem(j, LAGS[0] + 1)] = both[half:]

    @pl.when((j >= LAGS[0]) & (j < n + LAGS[0]))
    def _():
        t = j - LAGS[0]
        for c in stage0(t):
            c.wait_recv()
        total = kept0[lax.rem(t, LAGS[0] + 1)] + in0[t].astype(F32)
        for p in range(2):
            out1[t, p] = total[4 * p * unit : (4 * p + 2) * unit].astype(BF16)
            kept1[lax.rem(t, 4), p] = total[(4 * p + 2) * unit : (4 * p + 4) * unit]
        for c in stage1(t):
            c.start()

    @pl.when((j >= LAGS[1]) & (j < n + LAGS[1]))
    def _():
        t = j - LAGS[1]
        for c in stage1(t):
            c.wait_recv()
        for p in range(2):
            total = kept1[lax.rem(t, 4), p] + in1[t, p].astype(F32)
            out2[t, p] = total[:unit].astype(BF16)
            kept2[lax.rem(t, 4), p] = total[unit:]
        for c in stage2(t):
            c.start()

    @pl.when(j >= LAGS[2])
    def _():
        t = j - LAGS[2]
        for c in stage2(t):
            c.wait_recv()
        columns = pl.ds(pl.multiple_of(t * tile, tile), tile)
        for p in range(2):
            total = kept2[lax.rem(t, 4), p] + in2[t, p].astype(F32)
            here = slice(p * unit, (p + 1) * unit)
            h_ref[here, columns] = (res_ref[here, columns].astype(F32) + total).astype(BF16)

    @pl.when(j == pl.num_programs(0) - 1)
    def _():
        if norm:
            wide = h_ref[...].astype(F32)
            scale = lax.rsqrt(jnp.mean(wide * wide, -1, keepdims=True) + 1e-6)
            b_ref[...] = (wide * scale * gain_ref[...].astype(F32)).astype(BF16)

        @pl.loop(0, n)
        def _(t):
            for c in stage0(t) + stage1(t) + stage2(t):
                c.wait_send()


def reduced(a, w, res, gain, tile, norm, collective_id):
    rows, k = a.shape
    d = w.shape[1]
    n, unit = d // tile, rows // 16
    fixed = lambda j: (0, 0)
    mine = jax.ShapeDtypeStruct((2 * unit, d), BF16)
    return pl.pallas_call(
        functools.partial(_reduced_kernel, norm=norm),
        grid=(n + LAGS[2],),
        in_specs=[pl.BlockSpec((rows, k), fixed), pl.BlockSpec((k, tile), lambda j: (0, jnp.minimum(j, n - 1))),
                  pl.BlockSpec((2 * unit, d), fixed), pl.BlockSpec((1, d), fixed)],
        out_specs=[pl.BlockSpec((2 * unit, d), fixed)] * (1 + norm),
        out_shape=[mine] * (1 + norm),
        scratch_shapes=[
            pltpu.VMEM((rows, k), BF16),
            pltpu.VMEM((LAGS[0] + 1, 8 * unit, tile), F32),
            pltpu.VMEM((4, 2, 2 * unit, tile), F32),
            pltpu.VMEM((4, 2, unit, tile), F32),
            pltpu.VMEM((n, 8 * unit, tile), BF16),
            pltpu.VMEM((n, 8 * unit, tile), BF16),
            pltpu.VMEM((n, 2, 2 * unit, tile), BF16),
            pltpu.VMEM((n, 2, 2 * unit, tile), BF16),
            pltpu.VMEM((n, 2, unit, tile), BF16),
            pltpu.VMEM((n, 2, unit, tile), BF16),
            pltpu.SemaphoreType.DMA((n,)),
            pltpu.SemaphoreType.DMA((n,)),
            pltpu.SemaphoreType.DMA((n, 2)),
            pltpu.SemaphoreType.DMA((n, 2)),
            pltpu.SemaphoreType.DMA((n, 2)),
            pltpu.SemaphoreType.DMA((n, 2)),
        ],
        compiler_params=pltpu.CompilerParams(dimension_semantics=("arbitrary",), vmem_limit_bytes=VMEM, collective_id=collective_id,
                                             has_side_effects=True),
        cost_estimate=pl.CostEstimate(flops=max(2 * rows * k * d, 2 * rows * 2560 * d), transcendentals=0, bytes_accessed=2 * (rows * k + k * d) + rows * d * 2),
        name=f"reduced{collective_id}",
    )(a, w, res, gain)


AT_ATTENTION = {0: (0, 3), 1: (3, 7), 2: (7, 11), 3: (11, 14)}
AT_GATE = {0: (0, 3), 2: (3, 7), 4: (7, 11), 6: (11, 14)}


def _fused_kernel(a_ref, w_ref, res_ref, gain_ref, act_ref, *rest, attention, norm, chunk, source, lag, after):
    more, rest = (rest[:6], rest[6 + after :]) if attention else (rest[:2], rest[2 + after :])
    o_ref, h_ref, rest = rest[0], rest[1], rest[2:]
    b_ref, rest = (rest[0], rest[1:]) if norm else (None, rest)
    rows_s, kept0, kept1, out0, in0, out1, in1, out2, in2, sent0, came0, sent1, came1, sent2, came2, loaded, act_sem, act_s = rest[:18]
    res_s, res_sem, rest = rest[18], rest[19], rest[20:]
    unit = a_ref.shape[0] // 16
    half, tile, n = 8 * unit, w_ref.shape[1], out0.shape[0]
    j = pl.program_id(0)
    x, y, core, mate, over_x, over_y = _neighbours()

    def stage0(t):
        return [_remote(out0.at[t], in0.at[t], sent0.at[t], came0.at[t], mate)]

    def stage1(t):
        return [_remote(out1.at[t, p], in1.at[t, p], sent1.at[t, p], came1.at[t, p], to) for p, to in enumerate((over_x, over_y))]

    def stage2(t):
        return [_remote(out2.at[t, p], in2.at[t, p], sent2.at[t, p], came2.at[t, p], to) for p, to in enumerate((over_y, over_x))]

    def loads():
        order = [(1 - x, 1 - y, 0), (1 - x, y, 0), (x, 1 - y, 0), (x, y, 0), (1 - x, 1 - y, 1), (x, 1 - y, 1), (1 - x, y, 1), (x, y, 1)]
        copies = []
        for i, (xx, yy, part) in enumerate(order):
            for k, cc in enumerate((1 - core, core)):
                at = pl.multiple_of((((xx * 2 + yy) * 2 + cc) * 2 + part) * unit, unit)
                to = (8 * k + i) * unit
                copies.append(pltpu.make_async_copy(a_ref.at[pl.ds(at, unit), :], rows_s.at[to : to + unit, :], loaded.at[8 * k + i]))
        return copies

    act = pltpu.make_async_copy(act_ref.at[chunk] if attention else act_ref, act_s, act_sem)
    if source is not None:
        res_ref = res_ref.at[source, pl.ds(pl.multiple_of(lax.axis_index("tp") * 2 * unit, 2 * unit), 2 * unit), :]
    res = pltpu.make_async_copy(res_ref, res_s, res_sem)
    if attention:
        gain_a, wk_ref, wv_ref, wq_ref, cos_ref, sin_ref = more
        kv_s, kv_sems, second_s, second_sems, k_s, vt_s = rest
        last_step = pl.cdiv(wq_ref.shape[1], 2 * HEAD)
        kv = [pltpu.make_async_copy(ref, kv_s.at[:, i * HEAD : (i + 1) * HEAD], kv_sems.at[i]) for i, ref in enumerate((wk_ref, wv_ref))]

        def weights(i):
            at = 2 * HEAD * i
            width = min(2 * HEAD, wq_ref.shape[1] - at)
            return [pltpu.make_async_copy(wq_ref.at[:, at : at + width], second_s.at[i % 2, :, :width], second_sems.at[i % 2])]

    else:
        g_ref, u_ref = more
        second_s, second_sems = rest
        step = second_s.shape[3]
        last_step = g_ref.shape[1] // step

        def weights(i):
            slot, here = lax.rem(i, 2), pl.ds(pl.multiple_of(i * step, step), step)
            return [pltpu.make_async_copy(ref.at[:, here], second_s.at[slot, k], second_sems.at[slot, k]) for k, ref in enumerate((g_ref, u_ref))]

    @pl.when(j == 0)
    def _():
        for c in loads():
            c.start()
        barrier = pltpu.get_barrier_semaphore()
        for to in (mate, over_x, over_y):
            pl.semaphore_signal(barrier, 1, device_id={"tp": to}, device_id_type=MESH)
        for c in loads():
            c.wait()
        pl.semaphore_wait(barrier, 3)

    @pl.when(j == 3)
    def _():
        act.start()
        if attention:
            for c in kv:
                c.start()
        for i in range(2):
            for c in weights(i):
                c.start()
        res.start()

    @pl.when(j < n)
    def _():
        both = _dot(rows_s[...], w_ref[...])
        out0[j] = both[:half].astype(BF16)
        for c in stage0(j):
            c.start()
        kept0[lax.rem(j, lag + 1)] = both[half:]

    @pl.when((j >= lag) & (j < n + lag))
    def _():
        t = j - lag
        for c in stage0(t):
            c.wait_recv()
        total = kept0[lax.rem(t, lag + 1)] + in0[t].astype(F32)
        for p in range(2):
            out1[t, p] = total[4 * p * unit : (4 * p + 2) * unit].astype(BF16)
            kept1[t, p] = total[(4 * p + 2) * unit : (4 * p + 4) * unit]
        for c in stage1(t):
            c.start()

    for at, (first, end) in (AT_ATTENTION if attention else AT_GATE).items():

        @pl.when(j == n + at)
        def _():
            @pl.loop(first, end)
            def _(t):
                for c in stage1(t):
                    c.wait_recv()
                for p in range(2):
                    total = kept1[t, p] + in1[t, p].astype(F32)
                    out2[t, p] = total[:unit].astype(BF16)
                    kept1[t, p, unit:, :] = total[unit:]
                for c in stage2(t):
                    c.start()

    @pl.when(j == n)
    def _():
        act.wait()

    if attention:

        @pl.when(j == n)
        def _():
            for c in kv:
                c.wait()
            _attend_first(lambda here: act_s[here, :], gain_a, lambda: kv_s[...], cos_ref, sin_ref, act_s, k_s, vt_s)

        for i in range(last_step):

            @pl.when(j == n + 1 + i)
            def _():
                for c in weights(i):
                    c.wait()

        @pl.when(j > n)
        def _():
            _attend_pair(second_s[lax.rem(j - n - 1, 2)], cos_ref, sin_ref, o_ref, act_s, k_s, vt_s)

        for i in range(2, last_step):

            @pl.when(j == n + i - 1)
            def _():
                for c in weights(i):
                    c.start()

    else:

        @pl.when(j >= n)
        def _():
            i = j - n
            for c in weights(i):
                c.wait()
            gate = _dot(act_s[...], second_s[lax.rem(i, 2), 0])
            up = _dot(act_s[...], second_s[lax.rem(i, 2), 1])
            o_ref[...] = (jax.nn.silu(gate) * up).astype(BF16)

            @pl.when(i + 2 < last_step)
            def _():
                for c in weights(i + 2):
                    c.start()

    @pl.when(j == pl.num_programs(0) - 1)
    def _():
        res.wait()

        @pl.loop(0, n)
        def _(t):
            for c in stage2(t):
                c.wait_recv()
            columns = pl.ds(pl.multiple_of(t * tile, tile), tile)
            for p in range(2):
                here = slice(p * unit, (p + 1) * unit)
                h_ref[here, columns] = (res_s[here, columns].astype(F32) + kept1[t, p, unit:, :] + in2[t, p].astype(F32)).astype(BF16)

        if norm:
            b_ref[...] = _normed(h_ref[...], gain_ref[...])

        @pl.loop(0, n)
        def _(t):
            for c in stage0(t) + stage1(t) + stage2(t):
                c.wait_send()


def fused(a, w, res, gain, norm, collective_id, *, source=None, chunk=None, attention=None, gate=None, after=(), tile=512):
    rows, k = a.shape
    d = w.shape[1]
    n, unit = d // tile, rows // 16
    fixed = lambda j: (0, 0)
    anywhere = pl.BlockSpec(memory_space=pl.ANY)
    dma = pltpu.SemaphoreType.DMA
    step = 2 * HEAD
    if attention is not None:
        act, gain_a, wq, wk, wv, cos, sin = attention
        width = wq.shape[1]
        inputs = [gain_a, wk, wv, wq, cos, sin]
        specs = [pl.BlockSpec((1, d), fixed), anywhere, anywhere, anywhere, pl.BlockSpec((rows, HEAD), fixed), pl.BlockSpec((rows, HEAD), fixed)]
        steps, ahead = pl.cdiv(width, step) + 1, n + 1
        scratch = [pltpu.VMEM((d, step), BF16), dma((2,)), pltpu.VMEM((2, d, step), BF16), dma((2,)), pltpu.VMEM((rows, HEAD), BF16),
                   pltpu.VMEM((HEAD, rows), BF16)]
        flops = 2 * rows * d * (width + step) + 4 * rows * rows * width
    else:
        act, *inputs = gate
        width = inputs[0].shape[1]
        specs = [anywhere, anywhere]
        steps, ahead = width // step, n
        scratch = [pltpu.VMEM((2, 2, d, step), BF16), dma((2, 2))]
        flops = 4 * rows * d * width
    lag = 3 if norm else 2
    mine = jax.ShapeDtypeStruct((2 * unit, d), BF16)
    return pl.pallas_call(
        functools.partial(_fused_kernel, attention=attention is not None, norm=norm, chunk=chunk, source=source, lag=lag, after=len(after)),
        grid=(n + steps,),
        in_specs=[anywhere, pl.BlockSpec((k, tile), lambda j: (0, jnp.minimum(j, n - 1))), anywhere, pl.BlockSpec((1, d), fixed), anywhere,
                  *specs, *[anywhere] * len(after)],
        out_specs=[pl.BlockSpec((rows, step), lambda j: (0, jnp.maximum(j - ahead, 0)))] + [pl.BlockSpec((2 * unit, d), fixed)] * (1 + norm),
        out_shape=[jax.ShapeDtypeStruct((rows, width), BF16)] + [mine] * (1 + norm),
        scratch_shapes=[
            pltpu.VMEM((rows, k), BF16),
            pltpu.VMEM((lag + 1, 8 * unit, tile), F32),
            pltpu.VMEM((n, 2, 2 * unit, tile), F32),
            *[pltpu.VMEM((n, 8 * unit, tile), BF16)] * 2,
            *[pltpu.VMEM((n, 2, 2 * unit, tile), BF16)] * 2,
            *[pltpu.VMEM((n, 2, unit, tile), BF16)] * 2,
            *[dma((n,))] * 2,
            *[dma((n, 2))] * 4,
            dma((16,)),
            dma,
            pltpu.VMEM((rows, d), BF16),
            pltpu.VMEM((2 * unit, d), BF16),
            dma,
            *scratch,
        ],
        compiler_params=pltpu.CompilerParams(dimension_semantics=("arbitrary",), vmem_limit_bytes=VMEM, collective_id=collective_id,
                                             has_side_effects=True),
        cost_estimate=pl.CostEstimate(flops=2 * rows * k * d + flops, transcendentals=0, bytes_accessed=4 * rows * d),
        name=f"fused{collective_id}",
    )(a, w, res, gain, act, *inputs, *after)


def _place_kernel(piece, *rest, chunk):
    whole, held, taken, put = rest[-4:]
    parts, block = held.shape[:2]
    there = lambda i: pl.ds(i * block, block)
    take = [pltpu.make_async_copy(piece.at[there(i), :], held.at[i], taken.at[i]) for i in range(parts)]
    give = [pltpu.make_async_copy(held.at[i], whole.at[chunk, there(i), :], put.at[i]) for i in range(parts)]
    for c in take:
        c.start()
    for a, b in zip(take, give):
        a.wait()
        b.start()
    for c in give:
        c.wait()


def placed(piece, whole, c, chunks):
    rows, d = piece.shape
    parts = 16
    more = [] if whole is None else [whole]
    anywhere = pl.BlockSpec(memory_space=pl.ANY)
    return pl.pallas_call(
        functools.partial(_place_kernel, chunk=c),
        in_specs=[anywhere] * (1 + len(more)),
        out_specs=anywhere,
        out_shape=jax.ShapeDtypeStruct((chunks, rows, d), piece.dtype),
        scratch_shapes=[pltpu.VMEM((parts, rows // parts, d), piece.dtype), *[pltpu.SemaphoreType.DMA((parts,))] * 2],
        input_output_aliases={1: 0} if more else {},
        compiler_params=pltpu.CompilerParams(vmem_limit_bytes=VMEM),
        cost_estimate=pl.CostEstimate(flops=rows * d * 64, transcendentals=0, bytes_accessed=4 * rows * d),
        name="placed",
    )(piece, *more)


ORDER = [("attention", 0), ("attention", 1), ("attention", 2), ("gate", 0), ("attention", 3), ("gate", 1), ("gate", 2), ("gate", 3)]


def solution(mesh):
    def step(x, gain_a, wq, wk, wv, wo, gain_m, w_gate, w_up, w_down):
        chunks, rows, d = x.shape
        half = HEAD // 2
        angle = jnp.arange(rows).astype(F32)[:, None] * THETA ** (-jnp.arange(half, dtype=F32) / half)
        cos, sin = jnp.cos(angle), jnp.sin(angle)
        cos, sin = jnp.concatenate([cos, cos], -1), jnp.concatenate([-sin, sin], -1)
        gain_a, gain_m = gain_a.reshape(1, d), gain_m.reshape(1, d)
        weights = (gain_a, wq, wk, wv, cos, sin)
        gathered = lambda t: lax.all_gather(t, "tp", axis=0, tiled=True)
        own, wholes, pieces = [None] * chunks, [None] * chunks, [None] * chunks
        last = attended(x, 0, *weights)
        for number, ((was, c), (kind, chunk)) in enumerate(zip(ORDER, ORDER[1:])):
            first = was == "attention"
            work = dict(attention=(x, *weights)) if kind == "attention" else dict(gate=(wholes[chunk], w_gate, w_up))
            after = [done[i] for done, i in {4: [(wholes, 2)], 5: [(pieces, 0)]}.get(number, ())]
            last, *got = fused(last, wo if first else w_down, x if first else own[c], gain_m, first, number, source=c if first else None,
                               chunk=chunk, after=after, **work)
            if first:
                own[c], wholes[c] = got[0], gathered(got[1])
            else:
                pieces[c] = gathered(got[0])
        c = ORDER[-1][1]
        pieces[c] = gathered(reduced(last, w_down, own[c], gain_m, 512, False, len(ORDER))[0])
        y = None
        for c in range(chunks):
            y = placed(pieces[c], y, c, chunks)
        return y

    tokens, whole, columns, rows_of = P("dp", None, None), P(None), P(None, "tp"), P("tp", None)
    return jax.shard_map(
        step,
        mesh=mesh,
        in_specs=(tokens, whole, columns, columns, columns, rows_of, whole, columns, columns, rows_of),
        out_specs=tokens,
        check_vma=False,
    )
```

```python
import functools

import jax
import jax.numpy as jnp
from jax import lax
from jax.experimental import pallas as pl
from jax.experimental.pallas import tpu as pltpu
from jax.sharding import PartitionSpec as P

HEAD = 128
THETA = 10000
LOG2E = 1.4426950408889634
HIDDEN = -1e30
VMEM = 60 * 2**20
MESH = pl.DeviceIdType.MESH
F32, BF16 = jnp.float32, jnp.bfloat16


def _dot(a, b, ca=1, cb=0):
    return lax.dot_general(a, b, (((ca,), (cb,)), ((), ())), preferred_element_type=F32)


def _neighbours():
    me = lax.axis_index("tp")
    x, y, core = me // 4, lax.rem(me // 2, 2), lax.rem(me, 2)
    return x, y, core, me + 1 - 2 * core, me + 4 - 8 * x, me + 2 - 4 * y


def _remote(src, dst, sent, came, to):
    return pltpu.make_async_remote_copy(src, dst, sent, came, device_id={"tp": to}, device_id_type=MESH)


def _normed(h, gain):
    wide = h.astype(F32)
    scale = lax.rsqrt(jnp.mean(wide * wide, -1, keepdims=True) + 1e-6)
    return (wide * scale * gain.astype(F32)).astype(BF16)


def _turn(t, cos, sin):
    t = t.astype(BF16).astype(F32)
    return (t * cos + pltpu.roll(t, HEAD // 2, 1) * sin).astype(BF16)


def _attend_first(take, gain_ref, wkv, cos_ref, sin_ref, a_s, k_s, vt_s):
    @pl.loop(0, a_s.shape[0] // 64)
    def _(i):
        here = pl.ds(pl.multiple_of(i * 64, 64), 64)
        a_s[here, :] = _normed(take(here), gain_ref[...])

    kv = _dot(a_s[...], wkv())
    k_s[...] = _turn(kv[:, :HEAD], cos_ref[...], sin_ref[...])
    vt_s[...] = kv[:, HEAD:].T.astype(BF16)


def _attend_pair(wq, cos_ref, sin_ref, o_ref, a_s, k_s, vt_s):
    rows, bq = a_s.shape[0], 256
    e = HEAD**-0.5 * LOG2E
    q2 = _dot(a_s[...], wq)
    seen = lax.broadcasted_iota(jnp.int32, (bq, bq), 0) <= lax.broadcasted_iota(jnp.int32, (bq, bq), 1)
    for n in range(2):
        q = _turn(q2[:, n * HEAD : (n + 1) * HEAD], cos_ref[...], sin_ref[...])
        for at in range(0, rows, bq):
            mine = q[at : at + bq]
            s = [_dot(k_s[j : j + bq, :], mine, 1, 1) for j in range(0, at + bq, bq)]
            s[-1] = jnp.where(seen, s[-1], HIDDEN)
            top = functools.reduce(jnp.maximum, [t.max(axis=0, keepdims=True) for t in s])
            p = [jnp.exp2((t - top) * e) for t in s]
            total = sum(t.sum(axis=0, keepdims=True) for t in p)
            sums = sum(_dot(vt_s[:, j * bq : (j + 1) * bq], t.astype(BF16)) for j, t in enumerate(p))
            o_ref[at : at + bq, n * HEAD : (n + 1) * HEAD] = (sums * (1 / total)).T.astype(BF16)


def _attend_kernel(x_ref, gain_ref, wk_ref, wv_ref, wq_ref, cos_ref, sin_ref, o_ref, a_s, k_s, vt_s):
    step = pl.program_id(0)

    @pl.when(step == 0)
    def _():
        wkv = lambda: jnp.concatenate([wk_ref[...], wv_ref[...]], axis=1)
        _attend_first(lambda here: x_ref[0, here, :], gain_ref, wkv, cos_ref, sin_ref, a_s, k_s, vt_s)

    @pl.when(step > 0)
    def _():
        _attend_pair(wq_ref[...], cos_ref, sin_ref, o_ref, a_s, k_s, vt_s)


def attended(x, c, gain, wq, wk, wv, cos, sin):
    rows, d = x.shape[1:]
    width = wq.shape[1]
    steps = pl.cdiv(width, 2 * HEAD) + 1
    later = lambda j: (0, jnp.maximum(j - 1, 0))
    fixed = lambda j: (0, 0)
    return pl.pallas_call(
        _attend_kernel,
        grid=(steps,),
        in_specs=[pl.BlockSpec((1, rows, d), lambda j: (c, 0, 0)), pl.BlockSpec((1, d), fixed), pl.BlockSpec((d, HEAD), fixed),
                  pl.BlockSpec((d, HEAD), fixed), pl.BlockSpec((d, 2 * HEAD), later), pl.BlockSpec((rows, HEAD), fixed), pl.BlockSpec((rows, HEAD), fixed)],
        out_specs=pl.BlockSpec((rows, 2 * HEAD), later),
        out_shape=jax.ShapeDtypeStruct((rows, width), BF16),
        scratch_shapes=[pltpu.VMEM((rows, d), BF16), pltpu.VMEM((rows, HEAD), BF16), pltpu.VMEM((HEAD, rows), BF16)],
        compiler_params=pltpu.CompilerParams(dimension_semantics=("arbitrary",), vmem_limit_bytes=VMEM),
        cost_estimate=pl.CostEstimate(flops=2 * rows * d * (width + 2 * HEAD) + 4 * rows * rows * width, transcendentals=0, bytes_accessed=4 * rows * d),
        name="attended",
    )(x, gain, wk, wv, wq, cos, sin)


LAGS = (1, 3, 5)


def _reduced_kernel(a_ref, w_ref, res_ref, gain_ref, h_ref, *rest, norm):
    b_ref, rest = (rest[0], rest[1:]) if norm else (None, rest)
    rows_s, kept0, kept1, kept2, out0, in0, out1, in1, out2, in2, sent0, came0, sent1, came1, sent2, came2 = rest
    unit = a_ref.shape[0] // 16
    half = 8 * unit
    tile = w_ref.shape[1]
    n = out0.shape[0]
    j = pl.program_id(0)
    me = lax.axis_index("tp")
    x, y, core = me // 4, lax.rem(me // 2, 2), lax.rem(me, 2)
    mate, over_x, over_y = me + 1 - 2 * core, me + 4 - 8 * x, me + 2 - 4 * y

    def remote(src, dst, sent, came, to):
        return pltpu.make_async_remote_copy(src, dst, sent, came, device_id={"tp": to}, device_id_type=MESH)

    def stage0(t):
        return [remote(out0.at[t], in0.at[t], sent0.at[t], came0.at[t], mate)]

    def stage1(t):
        return [remote(out1.at[t, p], in1.at[t, p], sent1.at[t, p], came1.at[t, p], to) for p, to in enumerate((over_x, over_y))]

    def stage2(t):
        return [remote(out2.at[t, p], in2.at[t, p], sent2.at[t, p], came2.at[t, p], to) for p, to in enumerate((over_y, over_x))]

    @pl.when(j == 0)
    def _():
        barrier = pltpu.get_barrier_semaphore()
        for to in (mate, over_x, over_y):
            pl.semaphore_signal(barrier, 1, device_id={"tp": to}, device_id_type=MESH)
        order = [(1 - x, 1 - y, 0), (1 - x, y, 0), (x, 1 - y, 0), (x, y, 0), (1 - x, 1 - y, 1), (x, 1 - y, 1), (1 - x, y, 1), (x, y, 1)]
        for i, (xx, yy, part) in enumerate(order):
            for k, cc in enumerate((1 - core, core)):
                at = pl.multiple_of((((xx * 2 + yy) * 2 + cc) * 2 + part) * unit, unit)
                rows_s[k * half + i * unit : k * half + (i + 1) * unit, :] = a_ref[pl.ds(at, unit), :]
        pl.semaphore_wait(barrier, 3)

    @pl.when(j < n)
    def _():
        both = _dot(rows_s[...], w_ref[...])
        out0[j] = both[:half].astype(BF16)
        for c in stage0(j):
            c.start()
        kept0[lax.rem(j, LAGS[0] + 1)] = both[half:]

    @pl.when((j >= LAGS[0]) & (j < n + LAGS[0]))
    def _():
        t = j - LAGS[0]
        for c in stage0(t):
            c.wait_recv()
        total = kept0[lax.rem(t, LAGS[0] + 1)] + in0[t].astype(F32)
        for p in range(2):
            out1[t, p] = total[4 * p * unit : (4 * p + 2) * unit].astype(BF16)
            kept1[lax.rem(t, 4), p] = total[(4 * p + 2) * unit : (4 * p + 4) * unit]
        for c in stage1(t):
            c.start()

    @pl.when((j >= LAGS[1]) & (j < n + LAGS[1]))
    def _():
        t = j - LAGS[1]
        for c in stage1(t):
            c.wait_recv()
        for p in range(2):
            total = kept1[lax.rem(t, 4), p] + in1[t, p].astype(F32)
            out2[t, p] = total[:unit].astype(BF16)
            kept2[lax.rem(t, 4), p] = total[unit:]
        for c in stage2(t):
            c.start()

    @pl.when(j >= LAGS[2])
    def _():
        t = j - LAGS[2]
        for c in stage2(t):
            c.wait_recv()
        columns = pl.ds(pl.multiple_of(t * tile, tile), tile)
        for p in range(2):
            total = kept2[lax.rem(t, 4), p] + in2[t, p].astype(F32)
            here = slice(p * unit, (p + 1) * unit)
            h_ref[here, columns] = (res_ref[here, columns].astype(F32) + total).astype(BF16)

    @pl.when(j == pl.num_programs(0) - 1)
    def _():
        if norm:
            wide = h_ref[...].astype(F32)
            scale = lax.rsqrt(jnp.mean(wide * wide, -1, keepdims=True) + 1e-6)
            b_ref[...] = (wide * scale * gain_ref[...].astype(F32)).astype(BF16)

        @pl.loop(0, n)
        def _(t):
            for c in stage0(t) + stage1(t) + stage2(t):
                c.wait_send()


def reduced(a, w, res, gain, tile, norm, collective_id):
    rows, k = a.shape
    d = w.shape[1]
    n, unit = d // tile, rows // 16
    fixed = lambda j: (0, 0)
    mine = jax.ShapeDtypeStruct((2 * unit, d), BF16)
    return pl.pallas_call(
        functools.partial(_reduced_kernel, norm=norm),
        grid=(n + LAGS[2],),
        in_specs=[pl.BlockSpec((rows, k), fixed), pl.BlockSpec((k, tile), lambda j: (0, jnp.minimum(j, n - 1))),
                  pl.BlockSpec((2 * unit, d), fixed), pl.BlockSpec((1, d), fixed)],
        out_specs=[pl.BlockSpec((2 * unit, d), fixed)] * (1 + norm),
        out_shape=[mine] * (1 + norm),
        scratch_shapes=[
            pltpu.VMEM((rows, k), BF16),
            pltpu.VMEM((LAGS[0] + 1, 8 * unit, tile), F32),
            pltpu.VMEM((4, 2, 2 * unit, tile), F32),
            pltpu.VMEM((4, 2, unit, tile), F32),
            pltpu.VMEM((n, 8 * unit, tile), BF16),
            pltpu.VMEM((n, 8 * unit, tile), BF16),
            pltpu.VMEM((n, 2, 2 * unit, tile), BF16),
            pltpu.VMEM((n, 2, 2 * unit, tile), BF16),
            pltpu.VMEM((n, 2, unit, tile), BF16),
            pltpu.VMEM((n, 2, unit, tile), BF16),
            pltpu.SemaphoreType.DMA((n,)),
            pltpu.SemaphoreType.DMA((n,)),
            pltpu.SemaphoreType.DMA((n, 2)),
            pltpu.SemaphoreType.DMA((n, 2)),
            pltpu.SemaphoreType.DMA((n, 2)),
            pltpu.SemaphoreType.DMA((n, 2)),
        ],
        compiler_params=pltpu.CompilerParams(dimension_semantics=("arbitrary",), vmem_limit_bytes=VMEM, collective_id=collective_id,
                                             has_side_effects=True),
        cost_estimate=pl.CostEstimate(flops=max(2 * rows * k * d, 2 * rows * 2560 * d), transcendentals=0, bytes_accessed=2 * (rows * k + k * d) + rows * d * 2),
        name=f"reduced{collective_id}",
    )(a, w, res, gain)


AT_ATTENTION = (0, 1, 2, 3)
AT_GATE = (0, 2, 4, 6)


def _fused_kernel(a_ref, w_ref, res_ref, gain_ref, act_ref, *rest, attention, norm, chunk, source, lag, after):
    more, rest = (rest[:6], rest[6 + after :]) if attention else (rest[:2], rest[2 + after :])
    o_ref, h_ref, rest = rest[0], rest[1], rest[2:]
    b_ref, rest = (rest[0], rest[1:]) if norm else (None, rest)
    rows_s, kept0, kept1, out0, in0, out1, in1, out2, in2, sent0, came0, sent1, came1, sent2, came2, loaded, act_sem, act_s = rest[:18]
    res_s, res_sem, rest = rest[18], rest[19], rest[20:]
    unit = a_ref.shape[0] // 16
    half, tile, n = 8 * unit, w_ref.shape[1], out0.shape[0]
    j = pl.program_id(0)
    x, y, core, mate, over_x, over_y = _neighbours()

    def stage0(t):
        return [_remote(out0.at[t], in0.at[t], sent0.at[t], came0.at[t], mate)]

    def stage1(t):
        return [_remote(out1.at[t, p], in1.at[t, p], sent1.at[t, p], came1.at[t, p], to) for p, to in enumerate((over_x, over_y))]

    def stage2(t):
        return [_remote(out2.at[t, p], in2.at[t, p], sent2.at[t, p], came2.at[t, p], to) for p, to in enumerate((over_y, over_x))]

    def loads():
        order = [(1 - x, 1 - y, 0), (1 - x, y, 0), (x, 1 - y, 0), (x, y, 0), (1 - x, 1 - y, 1), (x, 1 - y, 1), (1 - x, y, 1), (x, y, 1)]
        copies = []
        for i, (xx, yy, part) in enumerate(order):
            for k, cc in enumerate((1 - core, core)):
                at = pl.multiple_of((((xx * 2 + yy) * 2 + cc) * 2 + part) * unit, unit)
                to = (8 * k + i) * unit
                copies.append(pltpu.make_async_copy(a_ref.at[pl.ds(at, unit), :], rows_s.at[to : to + unit, :], loaded.at[8 * k + i]))
        return copies

    act = pltpu.make_async_copy(act_ref.at[chunk] if attention else act_ref, act_s, act_sem)
    if source is not None:
        res_ref = res_ref.at[source, pl.ds(pl.multiple_of(lax.axis_index("tp") * 2 * unit, 2 * unit), 2 * unit), :]
    res = pltpu.make_async_copy(res_ref, res_s, res_sem)
    if attention:
        gain_a, wk_ref, wv_ref, wq_ref, cos_ref, sin_ref = more
        kv_s, kv_sems, second_s, second_sems, k_s, vt_s = rest
        last_step = pl.cdiv(wq_ref.shape[1], 2 * HEAD)
        kv = [pltpu.make_async_copy(ref, kv_s.at[:, i * HEAD : (i + 1) * HEAD], kv_sems.at[i]) for i, ref in enumerate((wk_ref, wv_ref))]

        def weights(i):
            at = 2 * HEAD * i
            width = min(2 * HEAD, wq_ref.shape[1] - at)
            return [pltpu.make_async_copy(wq_ref.at[:, at : at + width], second_s.at[i % 2, :, :width], second_sems.at[i % 2])]

    else:
        g_ref, u_ref = more
        second_s, second_sems = rest
        step = second_s.shape[3]
        last_step = g_ref.shape[1] // step

        def weights(i):
            slot, here = lax.rem(i, 2), pl.ds(pl.multiple_of(i * step, step), step)
            return [pltpu.make_async_copy(ref.at[:, here], second_s.at[slot, k], second_sems.at[slot, k]) for k, ref in enumerate((g_ref, u_ref))]

    @pl.when(j == 0)
    def _():
        for c in loads():
            c.start()
        barrier = pltpu.get_barrier_semaphore()
        for to in (mate, over_x, over_y):
            pl.semaphore_signal(barrier, 1, device_id={"tp": to}, device_id_type=MESH)
        for c in loads():
            c.wait()
        pl.semaphore_wait(barrier, 3)

    @pl.when(j == 3)
    def _():
        act.start()
        if attention:
            for c in kv:
                c.start()
        for i in range(2):
            for c in weights(i):
                c.start()
        res.start()

    @pl.when(j < n)
    def _():
        both = _dot(rows_s[...], w_ref[...])
        out0[j] = both[:half].astype(BF16)
        for c in stage0(j):
            c.start()
        kept0[lax.rem(j, lag + 1)] = both[half:]

    @pl.when((j >= lag) & (j < n + lag))
    def _():
        t = j - lag
        for c in stage0(t):
            c.wait_recv()
        total = kept0[lax.rem(t, lag + 1)] + in0[t].astype(F32)
        for p in range(2):
            out1[t, p] = total[4 * p * unit : (4 * p + 2) * unit].astype(BF16)
            kept1[t, p] = total[(4 * p + 2) * unit : (4 * p + 4) * unit]
        for c in stage1(t):
            c.start()

    for quarter, at in enumerate(AT_ATTENTION if attention else AT_GATE):
        first, end = quarter * n // 4, (quarter + 1) * n // 4

        @pl.when(j == n + at)
        def _():
            @pl.loop(first, end)
            def _(t):
                for c in stage1(t):
                    c.wait_recv()
                for p in range(2):
                    total = kept1[t, p] + in1[t, p].astype(F32)
                    out2[t, p] = total[:unit].astype(BF16)
                    kept1[t, p, unit:, :] = total[unit:]
                for c in stage2(t):
                    c.start()

    @pl.when(j == n)
    def _():
        act.wait()

    if attention:

        @pl.when(j == n)
        def _():
            for c in kv:
                c.wait()
            _attend_first(lambda here: act_s[here, :], gain_a, lambda: kv_s[...], cos_ref, sin_ref, act_s, k_s, vt_s)

        for i in range(last_step):

            @pl.when(j == n + 1 + i)
            def _():
                for c in weights(i):
                    c.wait()

        @pl.when(j > n)
        def _():
            _attend_pair(second_s[lax.rem(j - n - 1, 2)], cos_ref, sin_ref, o_ref, act_s, k_s, vt_s)

        for i in range(2, last_step):

            @pl.when(j == n + i - 1)
            def _():
                for c in weights(i):
                    c.start()

    else:

        @pl.when(j >= n)
        def _():
            i = j - n
            for c in weights(i):
                c.wait()
            gate = _dot(act_s[...], second_s[lax.rem(i, 2), 0])
            up = _dot(act_s[...], second_s[lax.rem(i, 2), 1])
            o_ref[...] = (jax.nn.silu(gate) * up).astype(BF16)

            @pl.when(i + 2 < last_step)
            def _():
                for c in weights(i + 2):
                    c.start()

    @pl.when(j == pl.num_programs(0) - 1)
    def _():
        res.wait()

        @pl.loop(0, n)
        def _(t):
            for c in stage2(t):
                c.wait_recv()
            columns = pl.ds(pl.multiple_of(t * tile, tile), tile)
            for p in range(2):
                here = slice(p * unit, (p + 1) * unit)
                h_ref[here, columns] = (res_s[here, columns].astype(F32) + kept1[t, p, unit:, :] + in2[t, p].astype(F32)).astype(BF16)

        if norm:
            b_ref[...] = _normed(h_ref[...], gain_ref[...])

        @pl.loop(0, n)
        def _(t):
            for c in stage0(t) + stage1(t) + stage2(t):
                c.wait_send()


def fused(a, w, res, gain, norm, collective_id, *, source=None, chunk=None, attention=None, gate=None, after=()):
    rows, k = a.shape
    d = w.shape[1]
    tile = 1024 if norm else 512
    n, unit = d // tile, rows // 16
    fixed = lambda j: (0, 0)
    anywhere = pl.BlockSpec(memory_space=pl.ANY)
    dma = pltpu.SemaphoreType.DMA
    step = 2 * HEAD
    if attention is not None:
        act, gain_a, wq, wk, wv, cos, sin = attention
        width = wq.shape[1]
        inputs = [gain_a, wk, wv, wq, cos, sin]
        specs = [pl.BlockSpec((1, d), fixed), anywhere, anywhere, anywhere, pl.BlockSpec((rows, HEAD), fixed), pl.BlockSpec((rows, HEAD), fixed)]
        steps, ahead = pl.cdiv(width, step) + 1, n + 1
        scratch = [pltpu.VMEM((d, step), BF16), dma((2,)), pltpu.VMEM((2, d, step), BF16), dma((2,)), pltpu.VMEM((rows, HEAD), BF16),
                   pltpu.VMEM((HEAD, rows), BF16)]
        flops = 2 * rows * d * (width + step) + 4 * rows * rows * width
    else:
        act, *inputs = gate
        width = inputs[0].shape[1]
        specs = [anywhere, anywhere]
        steps, ahead = width // step, n
        scratch = [pltpu.VMEM((2, 2, d, step), BF16), dma((2, 2))]
        flops = 4 * rows * d * width
    lag = 1 if norm else 2
    mine = jax.ShapeDtypeStruct((2 * unit, d), BF16)
    return pl.pallas_call(
        functools.partial(_fused_kernel, attention=attention is not None, norm=norm, chunk=chunk, source=source, lag=lag, after=len(after)),
        grid=(n + steps,),
        in_specs=[anywhere, pl.BlockSpec((k, tile), lambda j: (0, jnp.minimum(j, n - 1))), anywhere, pl.BlockSpec((1, d), fixed), anywhere,
                  *specs, *[anywhere] * len(after)],
        out_specs=[pl.BlockSpec((rows, step), lambda j: (0, jnp.maximum(j - ahead, 0)))] + [pl.BlockSpec((2 * unit, d), fixed)] * (1 + norm),
        out_shape=[jax.ShapeDtypeStruct((rows, width), BF16)] + [mine] * (1 + norm),
        scratch_shapes=[
            pltpu.VMEM((rows, k), BF16),
            pltpu.VMEM((lag + 1, 8 * unit, tile), F32),
            pltpu.VMEM((n, 2, 2 * unit, tile), F32),
            *[pltpu.VMEM((n, 8 * unit, tile), BF16)] * 2,
            *[pltpu.VMEM((n, 2, 2 * unit, tile), BF16)] * 2,
            *[pltpu.VMEM((n, 2, unit, tile), BF16)] * 2,
            *[dma((n,))] * 2,
            *[dma((n, 2))] * 4,
            dma((16,)),
            dma,
            pltpu.VMEM((rows, d), BF16),
            pltpu.VMEM((2 * unit, d), BF16),
            dma,
            *scratch,
        ],
        compiler_params=pltpu.CompilerParams(dimension_semantics=("arbitrary",), vmem_limit_bytes=VMEM, collective_id=collective_id,
                                             has_side_effects=True),
        cost_estimate=pl.CostEstimate(flops=2 * rows * k * d + flops, transcendentals=0, bytes_accessed=4 * rows * d),
        name=f"fused{collective_id}",
    )(a, w, res, gain, act, *inputs, *after)


def _place_kernel(piece, *rest, chunk):
    whole, held, taken, put = rest[-4:]
    parts, block = held.shape[:2]
    there = lambda i: pl.ds(i * block, block)
    take = [pltpu.make_async_copy(piece.at[there(i), :], held.at[i], taken.at[i]) for i in range(parts)]
    give = [pltpu.make_async_copy(held.at[i], whole.at[chunk, there(i), :], put.at[i]) for i in range(parts)]
    for c in take:
        c.start()
    for a, b in zip(take, give):
        a.wait()
        b.start()
    for c in give:
        c.wait()


def placed(piece, whole, c, chunks):
    rows, d = piece.shape
    parts = 16
    more = [] if whole is None else [whole]
    anywhere = pl.BlockSpec(memory_space=pl.ANY)
    return pl.pallas_call(
        functools.partial(_place_kernel, chunk=c),
        in_specs=[anywhere] * (1 + len(more)),
        out_specs=anywhere,
        out_shape=jax.ShapeDtypeStruct((chunks, rows, d), piece.dtype),
        scratch_shapes=[pltpu.VMEM((parts, rows // parts, d), piece.dtype), *[pltpu.SemaphoreType.DMA((parts,))] * 2],
        input_output_aliases={1: 0} if more else {},
        compiler_params=pltpu.CompilerParams(vmem_limit_bytes=VMEM),
        cost_estimate=pl.CostEstimate(flops=rows * d * 64, transcendentals=0, bytes_accessed=4 * rows * d),
        name="placed",
    )(piece, *more)


ORDER = [("attention", 0), ("attention", 1), ("attention", 2), ("gate", 0), ("attention", 3), ("gate", 1), ("gate", 2), ("gate", 3)]


def solution(mesh):
    def step(x, gain_a, wq, wk, wv, wo, gain_m, w_gate, w_up, w_down):
        chunks, rows, d = x.shape
        half = HEAD // 2
        angle = jnp.arange(rows).astype(F32)[:, None] * THETA ** (-jnp.arange(half, dtype=F32) / half)
        cos, sin = jnp.cos(angle), jnp.sin(angle)
        cos, sin = jnp.concatenate([cos, cos], -1), jnp.concatenate([-sin, sin], -1)
        gain_a, gain_m = gain_a.reshape(1, d), gain_m.reshape(1, d)
        weights = (gain_a, wq, wk, wv, cos, sin)
        gathered = lambda t: lax.all_gather(t, "tp", axis=0, tiled=True)
        own, wholes, pieces = [None] * chunks, [None] * chunks, [None] * chunks
        last = attended(x, 0, *weights)
        for number, ((was, c), (kind, chunk)) in enumerate(zip(ORDER, ORDER[1:])):
            first = was == "attention"
            work = dict(attention=(x, *weights)) if kind == "attention" else dict(gate=(wholes[chunk], w_gate, w_up))
            after = [done[i] for done, i in {4: [(wholes, 2)], 5: [(pieces, 0)]}.get(number, ())]
            last, *got = fused(last, wo if first else w_down, x if first else own[c], gain_m, first, number, source=c if first else None,
                               chunk=chunk, after=after, **work)
            if first:
                own[c], wholes[c] = got[0], gathered(got[1])
            else:
                pieces[c] = gathered(got[0])
        c = ORDER[-1][1]
        pieces[c] = gathered(reduced(last, w_down, own[c], gain_m, 512, False, len(ORDER))[0])
        y = None
        for c in range(chunks):
            y = placed(pieces[c], y, c, chunks)
        return y

    tokens, whole, columns, rows_of = P("dp", None, None), P(None), P(None, "tp"), P("tp", None)
    return jax.shard_map(
        step,
        mesh=mesh,
        in_specs=(tokens, whole, columns, columns, columns, rows_of, whole, columns, columns, rows_of),
        out_specs=tokens,
        check_vma=False,
    )
```
